1024 devices in a mesh: row: 32 (over y, x_lo), col: 16 (over z, x_hi), layer: 2 (over core).
Axes of the slice: x: 8 (x_hi: 2, x_lo: 4; x = x_hi * 4 + x_lo), y: 8, z: 8, core: 2. Of those that a mesh axis runs over, the one named last changes fastest.
Arguments:
- hamiltonian: bfloat16 [32768, 32768], P('row', 'col'), as said below
- start_vectors: bfloat16 [256, 32768], P('row', ('col', 'layer')), may hold values from -6 to 6
- cut_low: float32 [1], replicated, may hold values from -1.6 to -1.2
- cut_high: float32 [1], replicated, may hold values from 2 to 2.4
Outputs:
- filtered: bfloat16 [256, 32768], P('row', ('col', 'layer'))
The draws below stay inside these ranges and needn't reach their ends.
Inputs may be any that keep to these rules, and one draw needn't show every extreme that they name: hamiltonian is exactly symmetric.
All inputs are finite; a program needn't handle non-finite values.
Results may differ from the reference program's by a relative error of at most 0.009.
Values may be sent and summed in bfloat16 or wider, within the bound.
A program may use at most 32 MiB of HBM per device.

```python
import jax
import jax.numpy as jnp
from jax import lax

K = 256
NH = 32768


def draw_hamiltonian(key, part):
    entries = jax.random.normal(key, (NH, NH), jnp.float32)
    row_ids = lax.broadcasted_iota(jnp.int32, (NH, NH), 0)
    col_ids = lax.broadcasted_iota(jnp.int32, (NH, NH), 1)
    symmetric = jnp.where(row_ids <= col_ids, entries, entries.T)
    return (symmetric * NH ** (-0.5)).astype(jnp.bfloat16)


def levels(key, shape, cuts, smallest, largest):
    gain, own = 1.0, jax.random.fold_in(key, 6)
    for dim, shards_of in cuts:
        heights = jnp.exp(jax.random.uniform(jax.random.fold_in(own, dim), (shards_of,), jnp.float32, smallest / len(cuts), largest / len(cuts)))
        gain = gain * jnp.repeat(heights, shape[dim] // shards_of).reshape([-1 if axis == dim else 1 for axis in range(len(shape))])
    return gain


def gaussian(key, dims, deviation, bound, split=(), kind=jnp.bfloat16):
    level = levels(key, dims, split, -0.22, 0.18) if split else 1.0
    values = jax.random.normal(key, dims, jnp.float32) * deviation * level
    return jnp.minimum(jnp.maximum(values, -bound), bound).astype(kind)


def setup_inputs(seed: int = 0) -> dict:
    seeds = jax.random.split(jax.random.key(seed), 5)
    return {
        "hamiltonian": draw_hamiltonian(jax.random.fold_in(seeds[4], 71), 0),
        "start_vectors": gaussian(seeds[1], (K, NH), 1.0, 6.0, ((0, 32), (1, 32))),
        "cut_low": jnp.clip(jax.random.uniform(seeds[2], (1,), jnp.float32, -1.6, -1.2), -1.6, -1.2),
        "cut_high": jnp.clip(jax.random.uniform(seeds[3], (1,), jnp.float32, 2.0, 2.4), 2.0, 2.4),
    }


def apply_shifted(vectors, hamiltonian, centre, half_width):
    block_rows = min(1024, NH)
    count = NH // block_rows

    def one_block(block_index):
        first_row = (block_index * block_rows).astype(jnp.int32)
        rows = lax.dynamic_slice_in_dim(hamiltonian, first_row, block_rows, 0).astype(jnp.float32)
        row_ids = lax.broadcasted_iota(jnp.int32, (block_rows, NH), 0) + first_row
        col_ids = lax.broadcasted_iota(jnp.int32, (block_rows, NH), 1)
        diagonal_mask = (row_ids == col_ids).astype(jnp.float32)
        shifted = ((rows - centre * diagonal_mask) / half_width).astype(jnp.bfloat16)
        return lax.dot_general(vectors, shifted, (((1,), (1,)), ((), ())), preferred_element_type=jnp.float32)

    pieces = lax.map(one_block, jnp.arange(count, dtype=jnp.int32))
    return jnp.transpose(pieces, (1, 0, 2)).reshape(vectors.shape[0], NH)


def reference(hamiltonian, start_vectors, cut_low, cut_high):
    centre = (cut_low[0] + cut_high[0]) * 0.5
    half_width = (cut_high[0] - cut_low[0]) * 0.5
    first = apply_shifted(start_vectors, hamiltonian, centre, half_width).astype(jnp.bfloat16)
    second = (2.0 * apply_shifted(first, hamiltonian, centre, half_width) - start_vectors.astype(jnp.float32)).astype(jnp.bfloat16)
    third = (2.0 * apply_shifted(second, hamiltonian, centre, half_width) - first.astype(jnp.float32)).astype(jnp.bfloat16)
    filtered = (2.0 * apply_shifted(third, hamiltonian, centre, half_width) - second.astype(jnp.float32)).astype(jnp.bfloat16)
    return filtered
```

```python
import functools

import jax
import jax.numpy as jnp
from jax import lax
from jax.experimental import pallas as pl
from jax.experimental.pallas import tpu as pltpu
from jax.sharding import PartitionSpec as P

MESH = pl.DeviceIdType.MESH
F32, BF16 = jnp.float32, jnp.bfloat16
CHAINS = 2


def ds(start, size):
    return pl.ds(pl.multiple_of(start, size), size)


def kernel(low_ref, high_ref, h_hbm, start_ref, out_ref,
           h, raw, panel0, colsend, colrecv, colsum, pairsend, pairrecv, panel1,
           rowsend, rowrecv, panel2, lastsend, lastrecv,
           h_sem, s_start, r_start, s_own, r_own, s_cut, r_cut, s_pair, r_pair, s_all, r_all,
           s_row, r_row, s_full, r_full, s_last, r_last, s_lown, r_lown):
    r, c, l = lax.axis_index("row"), lax.axis_index("col"), lax.axis_index("layer")
    y, z, xh = r // 4, c // 2, c % 2
    mine = (y + r % 4) % 4
    my_core, my_k = mine // CHAINS, mine % CHAINS

    loads = [
        pltpu.make_async_copy(h_hbm.at[pl.ds(256 * i, 256)], h.at[pl.ds(256 * i, 256)], h_sem.at[i])
        for i in range(4)
    ]
    for load in loads:
        load.start()

    def send(src, dst, s_sem, r_sem, row, col, layer):
        pltpu.make_async_remote_copy(
            src_ref=src, dst_ref=dst, send_sem=s_sem, recv_sem=r_sem,
            device_id=(row, col, layer), device_id_type=MESH,
        ).start()

    def wait(ref, sem):
        pltpu.make_async_copy(ref, ref, sem).wait()

    def each(n, body):
        def step(i, carry):
            body(i)
            return carry

        lax.fori_loop(0, n, step, 0)

    barrier = pltpu.get_barrier_semaphore()

    def greet(row, col, layer):
        pl.semaphore_signal(barrier, inc=1, device_id=(row, col, layer), device_id_type=MESH)

    def greet_row(i):
        greet((r + i + 1) % 32, c, l)
        greet((r + i + 1) % 32, c, 1 - l)

    each(31, greet_row)
    greet(r, c, 1 - l)
    each(7, lambda i: greet(r, 2 * ((z + i + 1) % 8) + xh, l))
    greet(r, 2 * z + 1 - xh, l)
    pl.semaphore_wait(barrier, 71)

    landing = raw.at[my_k, y, :, ds(l * 1024, 1024)]
    each(31, lambda i: send(start_ref, landing, s_start, r_start.at[my_k], (r + i + 1) % 32, c, my_core))

    @pl.when(l == my_core)
    def _():
        raw[my_k, y, :, ds(l * 1024, 1024)] = start_ref[...]

    @pl.when(l != my_core)
    def _():
        send(start_ref, landing, s_own, r_own, r, c, my_core)

    low, high = low_ref[0], high_ref[0]
    centre = (low + high) * 0.5
    half_width = (high - low) * 0.5
    scale = 1.0 / half_width
    diag = [
        jnp.where((r // 2 == c) & (r % 2 == half), centre, 0.0) for half in range(2)
    ]

    for load in loads:
        load.wait()

    def take_start(k):
        own = 2 * l + k == mine

        @pl.when(own)
        def _():
            wait(raw.at[k, pl.ds(0, 7)], r_start.at[k])

            @pl.when(l == my_core)
            def _():
                wait(raw.at[k, y, :, ds((1 - l) * 1024, 1024)], r_own)

        @pl.when(jnp.logical_not(own))
        def _():
            wait(raw.at[k], r_start.at[k])

        for i in range(4):
            pair = jnp.concatenate([raw[k, 2 * i].astype(F32), raw[k, 2 * i + 1].astype(F32)], axis=0)
            panel0[k, 16 * i:16 * i + 16, :] = pair.astype(BF16)

    def by_columns(s, k, panel):
        for n in range(4):
            cols = slice(256 * n, 256 * n + 256)
            value = lax.dot_general(
                panel[k], h[cols, :], (((1,), (1,)), ((), ())), preferred_element_type=F32
            )
            for half in range(2):
                lo = 1024 * half + 256 * n
                value = value - diag[half] * panel[k, :, lo:lo + 256].astype(F32)
            colsend[s, k, :, cols] = value.astype(BF16)

        def to(i):
            other = (z + i + 1) % 8
            send(colsend.at[s, k, ds(16 * (other // 2), 16), ds(512 * (other % 2), 512)],
                 colrecv.at[s, k, z], s_cut.at[s, k], r_cut.at[s, k], r, 2 * other + xh, l)

        each(7, to)
        colrecv[s, k, z] = colsend[s, k, ds(16 * (z // 2), 16), ds(512 * (z % 2), 512)]

    def pair_up(s, k):
        wait(colrecv.at[s, k, pl.ds(0, 7)], r_cut.at[s, k])
        total = colrecv[s, k, 0].astype(F32)
        for i in range(1, 8):
            total = total + colrecv[s, k, i].astype(F32)
        colsum[s, k] = total
        pairsend[s, k] = total.astype(BF16)
        send(pairsend.at[s, k], pairrecv.at[s, k], s_pair.at[s, k], r_pair.at[s, k], r, 2 * z + 1 - xh, l)

    def spread_first(s, k):
        wait(pairrecv.at[s, k], r_pair.at[s, k])
        total = colsum[s, k] + pairrecv[s, k].astype(F32)
        rows, cols = ds(16 * (z // 2), 16), ds(512 * (z % 2), 512)
        if s == 0:
            value = scale * total
        else:
            value = 2.0 * scale * total - panel1[0, k, rows, cols].astype(F32)
        panel1[s, k, rows, cols] = value.astype(BF16)
        piece = panel1.at[s, k, rows, cols]
        each(7, lambda i: send(piece, piece, s_all.at[s, k], r_all.at[s, k], r, 2 * ((z + i + 1) % 8) + xh, l))

    def by_rows(s, k):
        wait(colrecv.at[s, k, pl.ds(0, 7)], r_all.at[s, k])
        own = 2 * l + k == mine
        for n in range(8):
            cols = slice(256 * n, 256 * n + 256)
            lo = (256 * n) % 1024
            value = jnp.dot(panel1[s, k], h[:, cols], preferred_element_type=F32)
            value = value - diag[n // 4] * panel1[s, k, :, lo:lo + 256].astype(F32)
            if s == 0:
                rowsend[k, :, cols] = value.astype(BF16)
            else:
                second = panel2[k, :, cols].astype(F32)
                for i in range(8):
                    rows = slice(8 * i, 8 * i + 8)
                    share = jnp.where(own & (y == i), half_width * 0.5, 0.0)
                    lastsend[k, i, :, cols] = (value[rows] - share * second[rows]).astype(BF16)

    def cut_rows(k):
        def to(i):
            other = (r + i + 1) % 32
            send(rowsend.at[k, ds(16 * (other // 8), 16), ds(256 * (other % 8), 256)],
                 rowrecv.at[k, r], s_row.at[k], r_row.at[k], other, c, l)

        each(31, to)
        rowrecv[k, r] = rowsend[k, ds(16 * (r // 8), 16), ds(256 * (r % 8), 256)]

    def spread_second(k):
        wait(rowrecv.at[k, pl.ds(0, 31)], r_row.at[k])
        total = rowrecv[k, 0].astype(F32)
        for i in range(1, 32):
            total = total + rowrecv[k, i].astype(F32)
        rows, cols = ds(16 * (r // 8), 16), ds(256 * (r % 8), 256)
        value = 2.0 * scale * total - panel0[k, rows, cols].astype(F32)
        panel2[k, rows, cols] = value.astype(BF16)
        piece = panel2.at[k, rows, cols]
        each(31, lambda i: send(piece, piece, s_full.at[k], r_full.at[k], (r + i + 1) % 32, c, l))

    def send_last(k):
        own = 2 * l + k == mine

        def to(i):
            py = (y + i) % 8
            other = 4 * py + (2 * l + k + 8 - py) % 4

            @pl.when(other != r)
            def _():
                for half in range(2):
                    send(lastsend.at[k, py, :, pl.ds(1024 * half, 1024)], lastrecv.at[r],
                         s_last.at[k], r_last, other, c, half)

        each(8, to)

        @pl.when(own)
        def _():
            lastrecv[r] = lastsend[k, y, :, ds(1024 * l, 1024)]
            send(lastsend.at[k, y, :, ds(1024 * (1 - l), 1024)], lastrecv.at[r], s_lown, r_lown, r, c, 1 - l)

    def begin(k):
        take_start(k)
        by_columns(0, k, panel0)

    each(CHAINS, begin)
    each(CHAINS, lambda k: pair_up(0, k))
    each(CHAINS, lambda k: spread_first(0, k))

    def middle(k):
        by_rows(0, k)
        cut_rows(k)

    each(CHAINS, middle)
    each(CHAINS, spread_second)

    def again(k):
        wait(rowrecv.at[k, pl.ds(0, 31)], r_full.at[k])
        by_columns(1, k, panel2)

    each(CHAINS, again)
    each(CHAINS, lambda k: pair_up(1, k))
    each(CHAINS, lambda k: spread_first(1, k))

    def finish(k):
        by_rows(1, k)
        send_last(k)

    each(CHAINS, finish)

    wait(lastrecv.at[pl.ds(0, 31)], r_last)

    @pl.when(l != my_core)
    def _():
        wait(lastrecv.at[31], r_lown)

    total = lastrecv[0].astype(F32)
    for i in range(1, 32):
        total = total + lastrecv[i].astype(F32)
    out_ref[...] = (2.0 * scale * total).astype(BF16)

    wait(lastrecv.at[pl.ds(0, 31)], s_start)

    @pl.when(l != my_core)
    def _():
        wait(start_ref, s_own)

    @pl.when(l == my_core)
    def _():
        wait(lastrecv.at[31], s_lown)

    def drain(k):
        for s in range(2):
            wait(colrecv.at[s, k, pl.ds(0, 7)], s_cut.at[s, k])
            wait(pairsend.at[s, k], s_pair.at[s, k])
            wait(colrecv.at[s, k, pl.ds(0, 7)], s_all.at[s, k])
        wait(rowrecv.at[k, pl.ds(0, 31)], s_row.at[k])
        wait(rowrecv.at[k, pl.ds(0, 31)], s_full.at[k])
        own = 2 * l + k == mine

        @pl.when(own)
        def _():
            wait(lastsend.at[k, pl.ds(0, 7)], s_last.at[k])

        @pl.when(jnp.logical_not(own))
        def _():
            wait(lastsend.at[k], s_last.at[k])

    each(CHAINS, drain)


def local(hamiltonian, start_vectors, cut_low, cut_high):
    vmem, dma = pltpu.VMEM, pltpu.SemaphoreType.DMA
    n = CHAINS
    return pl.pallas_call(
        kernel,
        out_shape=jax.ShapeDtypeStruct(start_vectors.shape, BF16),
        in_specs=[
            pl.BlockSpec(memory_space=pltpu.SMEM),
            pl.BlockSpec(memory_space=pltpu.SMEM),
            pl.BlockSpec(memory_space=pl.ANY),
            pl.BlockSpec(memory_space=pltpu.VMEM),
        ],
        out_specs=pl.BlockSpec(memory_space=pltpu.VMEM),
        scratch_shapes=[
            vmem((1024, 2048), BF16),
            vmem((n, 8, 8, 2048), BF16),
            vmem((n, 64, 2048), BF16),
            vmem((2, n, 64, 1024), BF16),
            vmem((2, n, 8, 16, 512), BF16),
            vmem((2, n, 16, 512), F32),
            vmem((2, n, 16, 512), BF16),
            vmem((2, n, 16, 512), BF16),
            vmem((2, n, 64, 1024), BF16),
            vmem((n, 64, 2048), BF16),
            vmem((n, 32, 16, 256), BF16),
            vmem((n, 64, 2048), BF16),
            vmem((n, 8, 8, 2048), BF16),
            vmem((32, 8, 1024), BF16),
            dma((4,)),
            dma, dma((n,)), dma, dma,
            dma((2, n)), dma((2, n)), dma((2, n)), dma((2, n)), dma((2, n)), dma((2, n)),
            dma((n,)), dma((n,)), dma((n,)), dma((n,)),
            dma((n,)), dma, dma, dma,
        ],
        compiler_params=pltpu.CompilerParams(
            collective_id=0, has_side_effects=True, vmem_limit_bytes=40 * 1024 * 1024
        ),
        name="filter",
    )(cut_low, cut_high, hamiltonian, start_vectors)


def solution(mesh):
    return jax.shard_map(
        local,
        mesh=mesh,
        in_specs=(P("row", "col"), P("row", ("col", "layer")), P(), P()),
        out_specs=P("row", ("col", "layer")),
        check_vma=False,
    )
```

```python
import functools

import jax
import jax.numpy as jnp
from jax import lax
from jax.experimental import pallas as pl
from jax.experimental.pallas import tpu as pltpu
from jax.sharding import PartitionSpec as P

MESH = pl.DeviceIdType.MESH
F32, BF16 = jnp.float32, jnp.bfloat16
CHAINS = 4


def ds(start, size):
    return pl.ds(pl.multiple_of(start, size), size)


def kernel(low_ref, high_ref, h_hbm, start_hbm, out_ref,
           h, start, startsend, raw, panel0, colsend, colrecv, colsum, pairsend, pairrecv, panel1,
           rowsend, rowrecv, panel2, lastsend, lastrecv,
           h_sem, start_sem, s_start, r_start, s_own, r_own, s_cut, r_cut, s_pair, r_pair, s_all, r_all,
           s_row, r_row, s_full, r_full, s_last, r_last, s_lown, r_lown):
    r, c, l = lax.axis_index("row"), lax.axis_index("col"), lax.axis_index("layer")
    y, z, xh = r // 4, c // 2, c % 2
    x = r % 4
    mine = (y + x) % 4
    my_core, my_sub = mine // 2, mine % 2

    loads = [
        pltpu.make_async_copy(h_hbm.at[pl.ds(256 * i, 256)], h.at[pl.ds(256 * i, 256)], h_sem.at[i])
        for i in range(4)
    ]
    load_start = pltpu.make_async_copy(start_hbm, start, start_sem)
    load_start.start()
    for load in loads:
        load.start()

    def send(src, dst, s_sem, r_sem, row, col, layer):
        pltpu.make_async_remote_copy(
            src_ref=src, dst_ref=dst, send_sem=s_sem, recv_sem=r_sem,
            device_id=(row, col, layer), device_id_type=MESH,
        ).start()

    def wait(ref, sem):
        pltpu.make_async_copy(ref, ref, sem).wait()

    def each(n, body):
        def step(i, carry):
            body(i)
            return carry

        lax.fori_loop(0, n, step, 0)

    def ring_other(me, i):
        return (me + 4 + (1 - 2 * (i % 2)) * ((i + 1) // 2)) % 8

    def each_ring(me, body):
        each(7, lambda i: body(ring_other(me, i)))

    def each_row(body):
        each(28, lambda i: body(4 * ring_other(y, i // 4) + (x + 2 + i) % 4))
        each(3, lambda i: body(4 * y + (x + 1 + (i + 1) % 3) % 4))

    barrier = pltpu.get_barrier_semaphore()

    def greet(row, col, layer):
        pl.semaphore_signal(barrier, inc=1, device_id=(row, col, layer), device_id_type=MESH)

    def greet_row(other):
        greet(other, c, l)
        greet(other, c, 1 - l)

    each_row(greet_row)
    each_ring(z, lambda other: greet(r, 2 * other + xh, l))
    greet(r, c, 1 - l)
    greet(r, 2 * z + 1 - xh, l)
    load_start.wait()
    for a in range(2):
        startsend[a] = start[...].astype(F32)[4 * a:4 * a + 4].astype(BF16)
    pl.semaphore_wait(barrier, 71)

    for a in range(2):
        landing = raw.at[2 * a + my_sub, y, :, ds(l * 1024, 1024)]
        each_row(lambda other: send(
            startsend.at[a], landing, s_start.at[a], r_start.at[2 * a + my_sub], other, c, my_core))

        @pl.when(l == my_core)
        def _():
            raw[2 * a + my_sub, y, :, ds(l * 1024, 1024)] = startsend[a]

        @pl.when(l != my_core)
        def _():
            send(startsend.at[a], landing, s_own.at[a], r_own.at[a], r, c, my_core)

    low, high = low_ref[0], high_ref[0]
    centre = (low + high) * 0.5
    half_width = (high - low) * 0.5
    scale = 1.0 / half_width
    diag = [
        jnp.where((r // 2 == c) & (r % 2 == half), centre, 0.0) for half in range(2)
    ]

    for load in loads:
        load.wait()

    def take_start(k):
        own = 2 * l + k % 2 == mine

        @pl.when(own)
        def _():
            wait(raw.at[k, pl.ds(0, 7)], r_start.at[k])

            @pl.when(l == my_core)
            def _():
                wait(raw.at[k, y, :, ds((1 - l) * 1024, 1024)], r_own.at[k // 2])

        @pl.when(jnp.logical_not(own))
        def _():
            wait(raw.at[k], r_start.at[k])

        for i in range(2):
            rows = jnp.concatenate([raw[k, 4 * i + j].astype(F32) for j in range(4)], axis=0)
            panel0[k, 16 * i:16 * i + 16, :] = rows.astype(BF16)

    def by_columns(s, k, panel):
        for n in range(4):
            cols = slice(256 * n, 256 * n + 256)
            value = lax.dot_general(
                panel[k], h[cols, :], (((1,), (1,)), ((), ())), preferred_element_type=F32
            )
            for half in range(2):
                lo = 1024 * half + 256 * n
                value = value - diag[half] * panel[k, :, lo:lo + 256].astype(F32)
            colsend[s, k, :, cols] = value.astype(BF16)

        def to(other):
            send(colsend.at[s, k, ds(16 * (other // 4), 16), ds(256 * (other % 4), 256)],
                 colrecv.at[s, k, z], s_cut.at[s, k], r_cut.at[s, k], r, 2 * other + xh, l)

        each_ring(z, to)
        colrecv[s, k, z] = colsend[s, k, ds(16 * (z // 4), 16), ds(256 * (z % 4), 256)]

    def pair_up(s, k):
        wait(colrecv.at[s, k, pl.ds(0, 7)], r_cut.at[s, k])
        total = colrecv[s, k, 0].astype(F32)
        for i in range(1, 8):
            total = total + colrecv[s, k, i].astype(F32)
        colsum[s, k] = total
        pairsend[s, k] = total.astype(BF16)
        send(pairsend.at[s, k], pairrecv.at[s, k], s_pair.at[s, k], r_pair.at[s, k], r, 2 * z + 1 - xh, l)

    def spread_first(s, k):
        wait(pairrecv.at[s, k], r_pair.at[s, k])
        total = colsum[s, k] + pairrecv[s, k].astype(F32)
        rows, cols = ds(16 * (z // 4), 16), ds(256 * (z % 4), 256)
        if s == 0:
            value = scale * total
        else:
            value = 2.0 * scale * total - panel1[0, k, rows, cols].astype(F32)
        panel1[s, k, rows, cols] = value.astype(BF16)
        piece = panel1.at[s, k, rows, cols]
        each_ring(z, lambda other: send(piece, piece, s_all.at[s, k], r_all.at[s, k], r, 2 * other + xh, l))

    def by_rows(s, k):
        wait(colrecv.at[s, k, pl.ds(0, 7)], r_all.at[s, k])
        own = 2 * l + k % 2 == mine
        for n in range(8):
            cols = slice(256 * n, 256 * n + 256)
            lo = (256 * n) % 1024
            value = jnp.dot(panel1[s, k], h[:, cols], preferred_element_type=F32)
            value = value - diag[n // 4] * panel1[s, k, :, lo:lo + 256].astype(F32)
            if s == 0:
                rowsend[k, :, cols] = value.astype(BF16)
            else:
                second = panel2[k, :, cols].astype(F32)
                holds = own & (lax.broadcasted_iota(jnp.int32, value.shape, 0) // 4 == y)
                value = value - jnp.where(holds, half_width * 0.5, 0.0) * second
                for i in range(8):
                    lastsend[k, i, :, cols] = value[4 * i:4 * i + 4].astype(BF16)

    def cut_rows(k):
        def to(other):
            send(rowsend.at[k, ds(16 * (other // 16), 16), ds(128 * (other % 16), 128)],
                 rowrecv.at[k, r], s_row.at[k], r_row.at[k], other, c, l)

        each_row(to)
        rowrecv[k, r] = rowsend[k, ds(16 * (r // 16), 16), ds(128 * (r % 16), 128)]

    def spread_second(k):
        wait(rowrecv.at[k, pl.ds(0, 31)], r_row.at[k])
        total = rowrecv[k, 0].astype(F32)
        for i in range(1, 32):
            total = total + rowrecv[k, i].astype(F32)
        rows, cols = ds(16 * (r // 16), 16), ds(128 * (r % 16), 128)
        value = 2.0 * scale * total - panel0[k, rows, cols].astype(F32)
        panel2[k, rows, cols] = value.astype(BF16)
        piece = panel2.at[k, rows, cols]
        each_row(lambda other: send(piece, piece, s_full.at[k], r_full.at[k], other, c, l))

    def send_last(k):
        own = 2 * l + k % 2 == mine

        def to(i):
            py = ring_other(y, i)
            other = 4 * py + (2 * l + k % 2 + 8 - py) % 4

            @pl.when(other != r)
            def _():
                for half in range(2):
                    send(lastsend.at[k, py, :, pl.ds(1024 * half, 1024)], lastrecv.at[k // 2, r],
                         s_last.at[k], r_last.at[k // 2], other, c, half)

        each(8, to)

        @pl.when(own)
        def _():
            lastrecv[k // 2, r] = lastsend[k, y, :, ds(1024 * l, 1024)]
            send(lastsend.at[k, y, :, ds(1024 * (1 - l), 1024)], lastrecv.at[k // 2, r],
                 s_lown.at[k // 2], r_lown.at[k // 2], r, c, 1 - l)

    def begin(k):
        take_start(k)
        by_columns(0, k, panel0)

    each(CHAINS, begin)
    each(CHAINS, lambda k: pair_up(0, k))
    each(CHAINS, lambda k: spread_first(0, k))

    def middle(k):
        by_rows(0, k)
        cut_rows(k)

    each(CHAINS, middle)
    each(CHAINS, spread_second)

    def again(k):
        wait(rowrecv.at[k, pl.ds(0, 31)], r_full.at[k])
        by_columns(1, k, panel2)

    each(CHAINS, again)
    each(CHAINS, lambda k: pair_up(1, k))
    each(CHAINS, lambda k: spread_first(1, k))

    def finish(k):
        by_rows(1, k)
        send_last(k)

    each(CHAINS, finish)

    parts = []
    for a in range(2):
        wait(lastrecv.at[a, pl.ds(0, 31)], r_last.at[a])

        @pl.when(l != my_core)
        def _():
            wait(lastrecv.at[a, 31], r_lown.at[a])

        total = lastrecv[a, 0].astype(F32)
        for i in range(1, 32):
            total = total + lastrecv[a, i].astype(F32)
        parts.append(2.0 * scale * total)
    out_ref[...] = jnp.concatenate(parts, axis=0).astype(BF16)

    for a in range(2):
        wait(lastrecv.at[a, pl.ds(0, 31)], s_start.at[a])

        @pl.when(l != my_core)
        def _():
            wait(startsend.at[a], s_own.at[a])

        @pl.when(l == my_core)
        def _():
            wait(lastrecv.at[a, 31], s_lown.at[a])

    def drain(k):
        for s in range(2):
            wait(colrecv.at[s, k, pl.ds(0, 7)], s_cut.at[s, k])
            wait(pairsend.at[s, k], s_pair.at[s, k])
            wait(colrecv.at[s, k, pl.ds(0, 7)], s_all.at[s, k])
        wait(rowrecv.at[k, pl.ds(0, 31)], s_row.at[k])
        wait(rowrecv.at[k, pl.ds(0, 31)], s_full.at[k])
        own = 2 * l + k % 2 == mine

        @pl.when(own)
        def _():
            wait(lastsend.at[k, pl.ds(0, 7)], s_last.at[k])

        @pl.when(jnp.logical_not(own))
        def _():
            wait(lastsend.at[k], s_last.at[k])

    each(CHAINS, drain)


def local(hamiltonian, start_vectors, cut_low, cut_high):
    vmem, dma = pltpu.VMEM, pltpu.SemaphoreType.DMA
    n = CHAINS
    return pl.pallas_call(
        kernel,
        out_shape=jax.ShapeDtypeStruct(start_vectors.shape, BF16),
        in_specs=[
            pl.BlockSpec(memory_space=pltpu.SMEM),
            pl.BlockSpec(memory_space=pltpu.SMEM),
            pl.BlockSpec(memory_space=pltpu.HBM),
            pl.BlockSpec(memory_space=pltpu.HBM),
        ],
        out_specs=pl.BlockSpec(memory_space=pltpu.VMEM),
        scratch_shapes=[
            vmem((1024, 2048), BF16),
            vmem((8, 1024), BF16),
            vmem((2, 4, 1024), BF16),
            vmem((n, 8, 4, 2048), BF16),
            vmem((n, 32, 2048), BF16),
            vmem((2, n, 32, 1024), BF16),
            vmem((2, n, 8, 16, 256), BF16),
            vmem((2, n, 16, 256), F32),
            vmem((2, n, 16, 256), BF16),
            vmem((2, n, 16, 256), BF16),
            vmem((2, n, 32, 1024), BF16),
            vmem((n, 32, 2048), BF16),
            vmem((n, 32, 16, 128), BF16),
            vmem((n, 32, 2048), BF16),
            vmem((n, 8, 4, 2048), BF16),
            vmem((2, 32, 4, 1024), BF16),
            dma((4,)), dma,
            dma((2,)), dma((n,)), dma((2,)), dma((2,)),
            dma((2, n)), dma((2, n)), dma((2, n)), dma((2, n)), dma((2, n)), dma((2, n)),
            dma((n,)), dma((n,)), dma((n,)), dma((n,)),
            dma((n,)), dma((2,)), dma((2,)), dma((2,)),
        ],
        compiler_params=pltpu.CompilerParams(
            collective_id=0, has_side_effects=True, vmem_limit_bytes=67_043_328
        ),
        name="filter",
    )(cut_low, cut_high, hamiltonian, start_vectors)


def solution(mesh):
    return jax.shard_map(
        local,
        mesh=mesh,
        in_specs=(P("row", "col"), P("row", ("col", "layer")), P(), P()),
        out_specs=P("row", ("col", "layer")),
        check_vma=False,
    )
```
